32 devices in a mesh: dp: 1 (over z), tp: 4 (over y), fsdp: 8 (over x, core).
Axes of the slice: x: 4, y: 4, z: 1, core: 2. Of those that a mesh axis runs over, the one named last changes fastest.
The devices are a block of a 4x4x8 slice.
Arguments:
- x: bfloat16 [32, 1024, 2048], P(('dp', 'fsdp'))
- w_query: bfloat16 [2, 2048, 2048], P(None, 'fsdp', 'tp')
- w_key: bfloat16 [2, 2048, 2048], P(None, 'fsdp', 'tp')
- w_value: bfloat16 [2, 2048, 2048], P(None, 'fsdp', 'tp')
- w_out: bfloat16 [2, 2048, 2048], P(None, 'tp', 'fsdp')
- w_gate: bfloat16 [2, 2048, 8192], P(None, 'fsdp', 'tp')
- w_up: bfloat16 [2, 2048, 8192], P(None, 'fsdp', 'tp')
- w_down: bfloat16 [2, 8192, 2048], P(None, 'tp', 'fsdp')
- q_norm_w: float32 [2, 2048], P(None, 'tp')
- k_norm_w: float32 [2, 2048], P(None, 'tp')
- attn_norm_w: float32 [2, 2048], P(None, 'fsdp')
- ffn_norm_w: float32 [2, 2048], P(None, 'fsdp')
Outputs:
- output 1: bfloat16 [32, 1024, 2048], P(('dp', 'fsdp'))
- output 2: bfloat16 [2, 32, 1024, 16, 128], P(None, ('dp', 'fsdp'), None, 'tp')
- output 3: bfloat16 [2, 32, 1024, 16, 128], P(None, ('dp', 'fsdp'), None, 'tp')
All inputs are finite; a program needn't handle non-finite values.
Results may differ from the reference program's by a relative error of at most 0.02.
Values are sent between devices in bfloat16 or wider.
A program may use at most 768 MiB of HBM per device.

```python
import jax
import jax.numpy as jnp
from jax import lax

MODEL_DIM = 2048
NUM_HEADS = 16
HEAD_DIM = 128
FF_DIM = 8192
BATCH_SIZE = 32
SEQ_LENGTH = 1024
NUM_LAYERS = 2
NORM_EPS = 1e-6
ROPE_THETA = 500000.0


def setup_inputs(seed: int = 0, part: int = 0) -> dict:
    keys = jax.random.split(jax.random.key(seed), 16)
    part_key = jax.random.fold_in(jax.random.key(seed + 1), part)
    dim_scale = MODEL_DIM ** -0.5
    ff_scale = FF_DIM ** -0.5
    square = (NUM_LAYERS, MODEL_DIM, MODEL_DIM)
    wide = (NUM_LAYERS, MODEL_DIM, FF_DIM)

    def normal_weight(key_w, shape_w, scale_w):
        return (jax.random.normal(key_w, shape_w, jnp.float32) * scale_w).astype(jnp.bfloat16)

    def head_scaled(key_w, key_s):
        weight = jax.random.normal(key_w, (NUM_LAYERS, MODEL_DIM, NUM_HEADS, HEAD_DIM), jnp.float32)
        scales = jnp.exp(jax.random.uniform(key_s, (NUM_LAYERS, 1, NUM_HEADS, 1), jnp.float32, -0.6, 0.6))
        return (weight * scales * dim_scale).reshape(square).astype(jnp.bfloat16)

    def gain(key_g):
        return jax.random.uniform(key_g, (NUM_LAYERS, MODEL_DIM), jnp.float32, 0.5, 1.5)

    x = jax.random.normal(part_key, (BATCH_SIZE, SEQ_LENGTH, MODEL_DIM), jnp.float32)
    return {
        'x': x.astype(jnp.bfloat16),
        'w_query': head_scaled(keys[0], keys[1]),
        'w_key': head_scaled(keys[2], keys[3]),
        'w_value': normal_weight(keys[4], square, dim_scale),
        'w_out': normal_weight(keys[5], square, dim_scale),
        'w_gate': normal_weight(keys[6], wide, dim_scale),
        'w_up': normal_weight(keys[7], wide, dim_scale),
        'w_down': normal_weight(keys[8], (NUM_LAYERS, FF_DIM, MODEL_DIM), ff_scale),
        'q_norm_w': gain(keys[9]),
        'k_norm_w': gain(keys[10]),
        'attn_norm_w': gain(keys[11]),
        'ffn_norm_w': gain(keys[12]),
    }


def rope_tables(seq_len):
    half = HEAD_DIM // 2
    inv_freq = ROPE_THETA ** (-2.0 * jnp.arange(half, dtype=jnp.float32) / HEAD_DIM)
    angles = jnp.arange(seq_len, dtype=jnp.float32)[:, None] * inv_freq[None, :]
    return jnp.cos(angles)[:, None, :], jnp.sin(angles)[:, None, :]


def apply_rope(vals, cos_t, sin_t):
    half = HEAD_DIM // 2
    first = vals[..., :half]
    second = vals[..., half:]
    return jnp.concatenate([first * cos_t - second * sin_t, second * cos_t + first * sin_t], axis=-1)


def rms_scale(vals):
    return lax.rsqrt(jnp.mean(vals * vals, axis=-1, keepdims=True) + NORM_EPS)


def attend_one(operands):
    q_seq, k_seq, v_seq = operands
    seq_len = q_seq.shape[0]
    scores = jnp.einsum('qhd,khd->hqk', q_seq.astype(jnp.float32), k_seq.astype(jnp.float32)) * (HEAD_DIM ** -0.5)
    causal = jnp.arange(seq_len)[:, None] >= jnp.arange(seq_len)[None, :]
    scores = jnp.where(causal[None, :, :], scores, -jnp.inf)
    attn_probs = jax.nn.softmax(scores, axis=-1).astype(jnp.bfloat16)
    result = jnp.einsum('hqk,khd->qhd', attn_probs.astype(jnp.float32), v_seq.astype(jnp.float32))
    return result.astype(jnp.bfloat16)


def layer_step(hidden, weights):
    w_query, w_key, w_value, w_out, w_gate, w_up, w_down, q_gain, k_gain, attn_gain, ffn_gain = weights
    batch, seq_len, width = hidden.shape
    flat = hidden.reshape(batch * seq_len, width)
    head_shape = (batch, seq_len, NUM_HEADS, HEAD_DIM)
    cos_t, sin_t = rope_tables(seq_len)
    q_raw = jnp.dot(flat, w_query, preferred_element_type=jnp.float32)
    k_raw = jnp.dot(flat, w_key, preferred_element_type=jnp.float32)
    values = jnp.dot(flat, w_value, preferred_element_type=jnp.float32).astype(jnp.bfloat16).reshape(head_shape)
    queries = apply_rope((q_raw * rms_scale(q_raw) * q_gain).reshape(head_shape), cos_t, sin_t).astype(jnp.bfloat16)
    keys_rot = apply_rope((k_raw * rms_scale(k_raw) * k_gain).reshape(head_shape), cos_t, sin_t).astype(jnp.bfloat16)
    attended = lax.map(attend_one, (queries, keys_rot, values))
    a_out = jnp.dot(attended.reshape(batch * seq_len, width), w_out, preferred_element_type=jnp.float32)
    a_out = a_out.astype(jnp.bfloat16).astype(jnp.float32)
    h_new = (flat.astype(jnp.float32) + a_out * rms_scale(a_out) * attn_gain).astype(jnp.bfloat16)
    gate = jnp.dot(h_new, w_gate, preferred_element_type=jnp.float32)
    up_val = jnp.dot(h_new, w_up, preferred_element_type=jnp.float32)
    hidden_act = (jax.nn.silu(gate) * up_val).astype(jnp.bfloat16)
    m_out = jnp.dot(hidden_act, w_down, preferred_element_type=jnp.float32)
    m_out = m_out.astype(jnp.bfloat16).astype(jnp.float32)
    result = (h_new.astype(jnp.float32) + m_out * rms_scale(m_out) * ffn_gain).astype(jnp.bfloat16)
    return result.reshape(batch, seq_len, width), (keys_rot, values)


def reference(x, w_query, w_key, w_value, w_out, w_gate, w_up, w_down, q_norm_w, k_norm_w, attn_norm_w, ffn_norm_w):
    stacked = (w_query, w_key, w_value, w_out, w_gate, w_up, w_down, q_norm_w, k_norm_w, attn_norm_w, ffn_norm_w)
    y, caches = lax.scan(layer_step, x, stacked)
    return y, caches[0], caches[1]
```

```python
import functools

import jax
import jax.numpy as jnp
from jax import lax
from jax.experimental import pallas as pl
from jax.experimental.pallas import tpu as pltpu
from jax.sharding import PartitionSpec as P

HEAD_DIM = 128
NORM_EPS = 1e-6
ROPE_THETA = 500000.0
CHUNKS = 2
QB = 256
F32, BF16 = jnp.float32, jnp.bfloat16


def rope_tables(seq_len):
    half = HEAD_DIM // 2
    inv_freq = ROPE_THETA ** (-2.0 * jnp.arange(half, dtype=F32) / HEAD_DIM)
    angles = jnp.arange(seq_len, dtype=F32)[:, None] * inv_freq[None, :]
    cos_t, sin_t = jnp.cos(angles), jnp.sin(angles)
    return jnp.concatenate([cos_t, cos_t], axis=-1), jnp.concatenate([-sin_t, sin_t], axis=-1)


def dot(a, b):
    return jnp.dot(a, b, preferred_element_type=F32)


def params(*semantics):
    return pltpu.CompilerParams(dimension_semantics=semantics or ("arbitrary",), vmem_limit_bytes=60 * 1024 * 1024)


def cost(flops, nbytes):
    return pl.CostEstimate(flops=flops, bytes_accessed=nbytes, transcendentals=0)


def rotate(vals, cos_t, sin_t):
    return vals * cos_t + pltpu.roll(vals, HEAD_DIM // 2, 1) * sin_t


def qkv_raw(x, w):
    tokens, width = x.shape
    part = w.shape[1] // 3
    tm = min(512, tokens)

    def body(x_ref, w_ref, q_ref, k_ref, v_ref, sq_ref):
        xb = x_ref[...]
        q = dot(xb, w_ref[:, :part])
        q_ref[...] = q
        q_sq = jnp.sum(q * q, axis=-1, keepdims=True)
        k = dot(xb, w_ref[:, part:2 * part])
        k_ref[...] = k
        k_sq = jnp.sum(k * k, axis=-1, keepdims=True)
        v_ref[...] = dot(xb, w_ref[:, 2 * part:]).astype(BF16)
        lane = lax.broadcasted_iota(jnp.int32, (tm, 128), 1)
        cols = jnp.where(lane == 0, q_sq, jnp.where(lane == 1, k_sq, 0.0))
        sq_ref[...] = cols.T[:8, :]

    row = lambda i: (i, 0)
    return pl.pallas_call(
        body, grid=(tokens // tm,),
        in_specs=[pl.BlockSpec((tm, width), row), pl.BlockSpec(w.shape, lambda i: (0, 0), pipeline_mode=pl.Buffered(1))],
        out_specs=[pl.BlockSpec((tm, part), row)] * 3 + [pl.BlockSpec((8, tm), lambda i: (0, i))],
        out_shape=[jax.ShapeDtypeStruct((tokens, part), d) for d in (F32, F32, BF16)]
        + [jax.ShapeDtypeStruct((8, tokens), F32)],
        compiler_params=params(), cost_estimate=cost(2 * tokens * width * 3 * part, 2 * tokens * width + 10 * tokens * part),
        name="qkv_raw")(x, w)


def norm_rope(q_raw, k_raw, inv, q_gain, k_gain, cos_t, sin_t):
    tokens, part = q_raw.shape
    tm = min(512, cos_t.shape[0])
    per_seq = cos_t.shape[0] // tm

    def body(q_ref, k_ref, inv_ref, qg_ref, kg_ref, cos_ref, sin_ref, qo_ref, ko_ref):
        for n, (src, gain, dst) in enumerate(((q_ref, qg_ref, qo_ref), (k_ref, kg_ref, ko_ref))):
            scale = jnp.broadcast_to(inv_ref[n:n + 1, :], (128, tm)).T
            for h in range(part // HEAD_DIM):
                cols = slice(h * HEAD_DIM, (h + 1) * HEAD_DIM)
                vals = src[:, cols] * scale * gain[:, cols]
                dst[:, cols] = rotate(vals, cos_ref[...], sin_ref[...]).astype(BF16)

    row = lambda i: (i, 0)
    gain = pl.BlockSpec((1, part), lambda i: (0, 0))
    table = pl.BlockSpec((tm, HEAD_DIM), lambda i: (lax.rem(i, per_seq), 0))
    return pl.pallas_call(
        body, grid=(tokens // tm,),
        in_specs=[pl.BlockSpec((tm, part), row)] * 2 + [pl.BlockSpec((8, tm), lambda i: (0, i)), gain, gain, table, table],
        out_specs=[pl.BlockSpec((tm, part), row)] * 2,
        out_shape=[jax.ShapeDtypeStruct((tokens, part), BF16)] * 2,
        compiler_params=params(), cost_estimate=cost(tokens * part * 2000, tokens * part * 12),
        name="norm_rope")(q_raw, k_raw, inv, q_gain, k_gain, cos_t, sin_t)


def softmax_pv(q, k, v, first):
    rows = q.shape[0]
    nt = (((1,), (1,)), ((), ()))
    scale = HEAD_DIM ** -0.5
    diag = lax.dot_general(q, k[first:], nt, preferred_element_type=F32) * scale
    keep = lax.broadcasted_iota(jnp.int32, (rows, rows), 0) >= lax.broadcasted_iota(jnp.int32, (rows, rows), 1)
    diag = jnp.where(keep, diag, -jnp.inf)
    top = jnp.max(diag, axis=-1, keepdims=True)
    if first:
        left = lax.dot_general(q, k[:first], nt, preferred_element_type=F32) * scale
        top = jnp.maximum(top, jnp.max(left, axis=-1, keepdims=True))
        p_left = jnp.exp(left - top)
    p_diag = jnp.exp(diag - top)
    total = jnp.sum(p_diag, axis=-1, keepdims=True)
    if first:
        total = total + jnp.sum(p_left, axis=-1, keepdims=True)
    inv = 1.0 / total
    out = dot((p_diag * inv).astype(BF16), v[first:])
    if first:
        out = out + dot((p_left * inv).astype(BF16), v[:first])
    return out.astype(BF16)


def attention(q, k, v, chunk, chunks, group):
    seqs, seq_len, width = q.shape
    qc = seq_len // chunks
    keys = qc * (chunk + 1)
    qb = min(QB, qc)
    heads = group // HEAD_DIM
    half = group // 2

    def body(q_ref, k_ref, v_ref, a_ref, b_ref):
        for h in range(heads):
            cols = slice(h * HEAD_DIM, (h + 1) * HEAD_DIM)
            dst = (a_ref, b_ref)[h * HEAD_DIM // half]
            dcols = slice(h * HEAD_DIM % half, h * HEAD_DIM % half + HEAD_DIM)
            for j in range(qc // qb):
                first = chunk * qc + j * qb
                last = first + qb
                dst[0, j * qb:(j + 1) * qb, dcols] = softmax_pv(
                    q_ref[0, j * qb:(j + 1) * qb, cols], k_ref[0, :last, cols], v_ref[0, :last, cols], first)

    groups = width // group
    kv = pl.BlockSpec((1, keys, group), lambda s, g: (s, 0, g))
    out = pl.BlockSpec((1, qc, half), lambda s, g: (s, 0, g))
    return pl.pallas_call(
        body, grid=(seqs, groups),
        in_specs=[pl.BlockSpec((1, qc, group), lambda s, g: (s, chunk, g)), kv, kv],
        out_specs=[out, out],
        out_shape=[jax.ShapeDtypeStruct((seqs, qc, groups * half), BF16)] * 2,
        compiler_params=params("arbitrary", "arbitrary"),
        cost_estimate=cost(8 * seqs * qc * keys * width, seqs * width * 2 * (2 * qc + 2 * keys)),
        name=f"attention_{chunk}_of_{chunks}")(q, k, v)


def out_proj_gathered(order, outs, w, x, gain, chunk, chunks):
    seqs, qc, half = outs[0].shape
    width = x.shape[2]
    shards, sources, rows, cols = w.shape

    def body(order_ref, *refs):
        o_refs, (w_ref, x_ref, gain_ref, h_ref, a_ref) = refs[:2 * sources], refs[2 * sources:]
        sq = jnp.zeros((qc, 1), F32)
        for f in range(shards):
            acc = jnp.zeros((qc, cols), F32)
            for s in range(sources):
                src = order_ref[s]
                acc += dot(o_refs[2 * s][0], w_ref[f, src, :half, :])
                acc += dot(o_refs[2 * s + 1][0], w_ref[f, src, half:, :])
            a = acc.astype(BF16)
            a_ref[:, f * cols:(f + 1) * cols] = a
            a = a.astype(F32)
            sq += jnp.sum(a * a, axis=-1, keepdims=True)
        inv = lax.rsqrt(sq / width + NORM_EPS)
        for f in range(shards):
            c = slice(f * cols, (f + 1) * cols)
            h_ref[0, :, c] = (x_ref[0, :, c].astype(F32) + a_ref[:, c].astype(F32) * inv * gain_ref[:, c]).astype(BF16)

    o_spec = pl.BlockSpec((1, qc, half), lambda r, order: (order[r], 0, 0))
    return pl.pallas_call(
        body,
        grid_spec=pltpu.PrefetchScalarGridSpec(
            num_scalar_prefetch=1, grid=(seqs,),
            in_specs=[o_spec] * (2 * sources) + [
                pl.BlockSpec(w.shape, lambda r, order: (0, 0, 0, 0), pipeline_mode=pl.Buffered(1)),
                pl.BlockSpec((1, qc, width), lambda r, order: (order[r], chunk, 0)),
                pl.BlockSpec((1, width), lambda r, order: (0, 0))],
            out_specs=pl.BlockSpec((1, qc, width), lambda r, order: (r, 0, 0)),
            scratch_shapes=[pltpu.VMEM((qc, width), BF16)]),
        out_shape=jax.ShapeDtypeStruct((seqs, qc, width), BF16),
        compiler_params=params(), cost_estimate=cost(2 * seqs * qc * width * width, 6 * seqs * qc * width + 2 * width * width),
        name=f"out_proj_{chunk}_of_{chunks}")(order, *outs, w, x, gain)


def mlp_part(h, w_gu, w_down, tag):
    seqs, qc, width = h.shape
    rows = seqs * qc
    ff = w_gu.shape[1] // 2
    shards, _, cols = w_down.shape
    tn = min(256, ff)
    up_steps = ff // tn
    halves = shards // 2

    def body(h_ref, g_ref, u_ref, d_ref, *refs):
        outs, act_ref = refs[:-1], refs[-1]
        step = pl.program_id(0)

        @pl.when(step < up_steps)
        def _():
            gate = dot(h_ref[...], g_ref[...])
            up = dot(h_ref[...], u_ref[...])
            act_ref[step] = (jax.nn.silu(gate) * up).astype(BF16)

        for side in range(2):
            @pl.when((step >= up_steps + side * halves) & (step < up_steps + (side + 1) * halves))
            def _(side=side):
                for s in range(seqs):
                    acc = jnp.zeros((qc, cols), F32)
                    for n in range(up_steps):
                        acc += dot(act_ref[n, s * qc:(s + 1) * qc, :], d_ref[0, n * tn:(n + 1) * tn, :])
                    outs[2 * s + side][...] = acc.astype(BF16)

    up_index = lambda i: jnp.minimum(i, up_steps - 1)
    down_index = lambda i: jnp.maximum(i - up_steps, 0)
    sides = (lambda i: (0, jnp.clip(i - up_steps, 0, halves - 1)), lambda i: (0, jnp.clip(i - up_steps - halves, 0, halves - 1)))
    return pl.pallas_call(
        body, grid=(up_steps + shards,),
        in_specs=[pl.BlockSpec((rows, width), lambda i: (0, 0), pipeline_mode=pl.Buffered(1)),
                  pl.BlockSpec((width, tn), lambda i: (0, up_index(i))),
                  pl.BlockSpec((width, tn), lambda i: (0, up_steps + up_index(i))),
                  pl.BlockSpec((1, ff, cols), lambda i: (down_index(i), 0, 0))],
        out_specs=[pl.BlockSpec((qc, cols), sides[side]) for _ in range(seqs) for side in range(2)],
        out_shape=[jax.ShapeDtypeStruct((qc, halves * cols), BF16)] * (2 * seqs),
        scratch_shapes=[pltpu.VMEM((up_steps, rows, tn), BF16)],
        compiler_params=params(), cost_estimate=cost(6 * rows * width * ff, 4 * rows * width + 6 * width * ff),
        name=f"mlp_part_{tag}")(h.reshape(rows, width), w_gu, w_gu, w_down)


def qkv_full(x, w, q_gain, k_gain, cos_t, sin_t, part):
    tokens, width = x.shape
    shards, tps, _, cols = w.shape
    depth = width // shards
    per = part // cols
    blocks = tps * per
    tr = min(256, tokens)

    def body(x_ref, w_ref, qg_ref, kg_ref, cos_ref, sin_ref, q_ref, k_ref, v_ref, raw_ref, sq_ref):
        which, n = pl.program_id(0), pl.program_id(1)
        out = dot(x_ref[...], w_ref[...].reshape(width, cols))

        @pl.when(which < 2)
        def _():
            raw_ref[n] = out
            part_sq = jnp.sum(out * out, axis=-1, keepdims=True)
            sq_ref[...] = jnp.where(n == 0, 0.0, sq_ref[...]) + part_sq

        @pl.when(which == 2)
        def _():
            v_ref[...] = out.astype(BF16)

        for sel, (gain, dst) in enumerate(((qg_ref, q_ref), (kg_ref, k_ref))):
            @pl.when((which == sel) & (n == blocks - 1))
            def _(gain=gain, dst=dst):
                def rows_body(r, _):
                    rows = pl.ds(r * tr, tr)
                    inv = lax.rsqrt(sq_ref[rows, :] / width + NORM_EPS)
                    for m in range(blocks):
                        for h in range(cols // HEAD_DIM):
                            lanes = slice(h * HEAD_DIM, (h + 1) * HEAD_DIM)
                            wide = slice(m * cols + h * HEAD_DIM, m * cols + (h + 1) * HEAD_DIM)
                            vals = raw_ref[m, rows, lanes] * inv * gain[:, wide]
                            dst[rows, wide] = rotate(vals, cos_ref[rows, :], sin_ref[rows, :]).astype(BF16)
                    return 0
                lax.fori_loop(0, tokens // tr, rows_body, 0)

    fixed = lambda s: pl.BlockSpec(s, lambda i, n: (0,) * len(s), pipeline_mode=pl.Buffered(1))
    whole = pl.BlockSpec((tokens, width), lambda i, n: (0, 0))
    return pl.pallas_call(
        body, grid=(3, blocks),
        in_specs=[fixed((tokens, width)),
                  pl.BlockSpec((shards, 1, depth, cols), lambda i, n: (0, n // per, i * per + n % per, 0)),
                  fixed((1, width)), fixed((1, width)), fixed(cos_t.shape), fixed(sin_t.shape)],
        out_specs=[whole, whole, pl.BlockSpec((tokens, cols), lambda i, n: (0, jnp.where(i == 2, n, 0)))],
        out_shape=[jax.ShapeDtypeStruct((tokens, width), BF16)] * 3,
        scratch_shapes=[pltpu.VMEM((blocks, tokens, cols), F32), pltpu.VMEM((tokens, 1), F32)],
        compiler_params=params("arbitrary", "arbitrary"),
        cost_estimate=cost(6 * tokens * width * width, 8 * tokens * width + 6 * width * width),
        name="qkv_full")(x, w, q_gain, k_gain, cos_t, sin_t)


def proj_norm(acts, w, row_block, x, gain, name):
    tokens, width = x.shape
    shards, tps, _, cols = w.shape
    depth = sum(a.shape[1] for a in acts) // tps
    tr = min(256, tokens)

    def body(*refs):
        a_refs, (w_ref, x_ref, gain_ref, out_ref, raw_ref, sq_ref) = refs[:len(acts)], refs[len(acts):]
        f = pl.program_id(0)
        if len(acts) == 1:
            out = dot(a_refs[0][...], w_ref[...].reshape(tps * depth, cols))
        else:
            out = jnp.zeros((tokens, cols), F32)
            half = depth // 2
            for t in range(tps):
                for side in range(2):
                    out += dot(a_refs[side][:, t * half:(t + 1) * half], w_ref[0, t, side * half:(side + 1) * half, :])
        out = out.astype(BF16)
        raw_ref[f] = out
        out = out.astype(F32)
        sq_ref[...] = jnp.where(f == 0, 0.0, sq_ref[...]) + jnp.sum(out * out, axis=-1, keepdims=True)

        @pl.when(f == shards - 1)
        def _():
            def rows_body(r, _):
                rows = pl.ds(r * tr, tr)
                inv = lax.rsqrt(sq_ref[rows, :] / width + NORM_EPS)
                for m in range(shards):
                    c = slice(m * cols, (m + 1) * cols)
                    out_ref[rows, c] = (x_ref[rows, c].astype(F32) + raw_ref[m, rows, :].astype(F32) * inv * gain_ref[:, c]).astype(BF16)
                return 0
            lax.fori_loop(0, tokens // tr, rows_body, 0)

    fixed = lambda s: pl.BlockSpec(s, lambda f: (0,) * len(s), pipeline_mode=pl.Buffered(1))
    return pl.pallas_call(
        body, grid=(shards,),
        in_specs=[fixed(a.shape) for a in acts] + [
            pl.BlockSpec((1, tps, depth, cols), lambda f: (f, 0, row_block, 0)), fixed((tokens, width)), fixed((1, width))],
        out_specs=pl.BlockSpec((tokens, width), lambda f: (0, 0)),
        out_shape=jax.ShapeDtypeStruct((tokens, width), BF16),
        scratch_shapes=[pltpu.VMEM((shards, tokens, cols), BF16), pltpu.VMEM((tokens, 1), F32)],
        compiler_params=params(),
        cost_estimate=cost(2 * tokens * tps * depth * width, 2 * tps * depth * (width + tokens)),
        name=name)(*acts, w, x, gain)


def gate_up(h, w):
    tokens, width = h.shape
    shards, tps, _, depth, ff = w.shape
    tn = min(256, ff)
    per = ff // tn

    def body(h_ref, g_ref, u_ref, act_ref):
        gate = dot(h_ref[...], g_ref[...].reshape(width, tn))
        up = dot(h_ref[...], u_ref[...].reshape(width, tn))
        act_ref[...] = (jax.nn.silu(gate) * up).astype(BF16)

    w_spec = lambda side: pl.BlockSpec((shards, 1, 1, depth, tn), lambda n: (0, n // per, side, 0, n % per))
    return pl.pallas_call(
        body, grid=(tps * per,),
        in_specs=[pl.BlockSpec((tokens, width), lambda n: (0, 0), pipeline_mode=pl.Buffered(1)), w_spec(0), w_spec(1)],
        out_specs=pl.BlockSpec((tokens, tn), lambda n: (0, n)),
        out_shape=jax.ShapeDtypeStruct((tokens, tps * ff), BF16),
        compiler_params=params(),
        cost_estimate=cost(4 * tokens * width * tps * ff, 4 * width * tps * ff + 2 * tokens * (width + tps * ff)),
        name="gate_up")(h, w, w)


def solution(mesh):
    batch_axes = ('dp', 'fsdp')
    act_spec = P(batch_axes, None, None)
    in_cols = P(None, 'fsdp', 'tp')
    in_rows = P(None, 'tp', 'fsdp')
    tp_gain = P(None, 'tp')
    fsdp_gain = P(None, 'fsdp')
    cache_spec = P(None, batch_axes, None, 'tp', None)
    tp = mesh.shape['tp']
    assert tp == 4
    ups = [(i, (i + 1) % tp) for i in range(tp)]
    downs = [(i, (i - 1) % tp) for i in range(tp)]
    everyone = ('fsdp', 'tp')

    def up(a):
        return lax.ppermute(a, 'tp', ups)

    def down(a):
        return lax.ppermute(a, 'tp', downs)

    def gather_all(a):
        g = lax.all_gather(a, everyone, axis=0, tiled=False)
        return g.reshape(mesh.shape['fsdp'], tp, *a.shape)

    def stacked_cols(w, cols):
        return [w[:, i:i + cols] for i in range(0, w.shape[1], cols)]

    def local_layers(x, w_query, w_key, w_value, w_out, w_gate, w_up, w_down, q_norm_w, k_norm_w, attn_norm_w, ffn_norm_w):
        batch, seq_len, width = x.shape
        assert batch == tp and w_query.shape[0] == 2
        tokens = batch * seq_len
        part = w_query.shape[2]
        cos_t, sin_t = rope_tables(seq_len)
        me = lax.axis_index('tp')
        seq_order = lax.rem(me + jnp.arange(tp, dtype=jnp.int32), tp)

        w_qkv = lax.all_gather(jnp.concatenate([w_query[0], w_key[0], w_value[0]], axis=1), 'fsdp', axis=0, tiled=True)
        fsdp_gains = lax.all_gather(jnp.stack([attn_norm_w, ffn_norm_w]), 'fsdp', axis=2, tiled=True)
        tp_gains = lax.all_gather(jnp.stack([q_norm_w[1], k_norm_w[1]]), 'tp', axis=1, tiled=True)
        w_o0 = gather_all(w_out[0])
        w_gu0 = lax.all_gather(jnp.concatenate([w_gate[0], w_up[0]], axis=1), 'fsdp', axis=0, tiled=True)
        w_d0 = lax.all_gather(w_down[0], 'fsdp', axis=0, tiled=False)
        cols = w_out.shape[2]
        w_attn1 = gather_all(jnp.concatenate(
            stacked_cols(w_query[1], cols) + stacked_cols(w_key[1], cols) + stacked_cols(w_value[1], cols) + [w_out[1]], axis=0))
        w_gu1 = gather_all(jnp.stack([w_gate[1], w_up[1]]))
        w_d1 = gather_all(w_down[1])

        q_raw, k_raw, values, sq = qkv_raw(x.reshape(tokens, width), w_qkv)
        sq_up, sq_down = up(sq), down(sq)
        sq_far = up(sq_up)
        inv = lax.rsqrt((sq + sq_up + sq_down + sq_far) / width + NORM_EPS)
        queries, keys_rot = norm_rope(q_raw, k_raw, inv, q_norm_w[:1], k_norm_w[:1], cos_t, sin_t)
        shape3 = (batch, seq_len, part)
        queries, keys_rot, values = (a.reshape(shape3) for a in (queries, keys_rot, values))
        mine = []
        for c in range(CHUNKS):
            own_a, own_b = attention(queries, keys_rot, values, c, CHUNKS, part)
            below_a, below_b = up(own_a), up(own_b)
            above_a, above_b = down(own_a), down(own_b)
            far_a, far_b = up(below_a), down(above_b)
            h = out_proj_gathered(seq_order, (own_a, own_b, above_a, above_b, far_a, far_b, below_a, below_b),
                                  w_o0, x, fsdp_gains[0, :1], c, CHUNKS)
            (p0a, p0b, p1a, p1b, p2a, p2b, p3a, p3b) = mlp_part(h, w_gu0, w_d0, c)
            r2a, r1b = up(p2a), up(p1b)
            r2b, r3a = down(p2b), down(p3a)
            r1a = up(p1a + r2a)
            r3b = down(p3b + r2b)
            m = jnp.concatenate([p0a.astype(F32) + r1a.astype(F32) + r3a.astype(F32),
                                 p0b.astype(F32) + r1b.astype(F32) + r3b.astype(F32)], axis=1)
            m = m.astype(BF16).astype(F32)
            scale = lax.rsqrt(jnp.mean(m * m, axis=-1, keepdims=True) + NORM_EPS)
            mine.append((h[0].astype(F32) + m * scale * fsdp_gains[1, :1]).astype(BF16))
        hidden = jnp.concatenate(mine, axis=0)

        def to_heads(a):
            return lax.all_to_all(a.reshape(seq_len, tp, part), 'tp', split_axis=1, concat_axis=0, tiled=False)

        q1, k1, v1 = qkv_full(hidden, w_attn1, tp_gains[:1], tp_gains[1:], cos_t, sin_t, part)
        k_heads, v_heads = to_heads(k1), to_heads(v1)
        o_a, o_b = attention(q1[None], k1[None], v1[None], 0, 1, part)
        h = proj_norm([o_a[0], o_b[0]], w_attn1, 3 * part // cols * (width // mesh.shape['fsdp']) // w_out.shape[1], hidden, fsdp_gains[0, 1:], "out_proj_full")
        act = gate_up(h, w_gu1)
        act, k_heads, v_heads = lax.optimization_barrier((act, k_heads, v_heads))
        y = proj_norm([act], w_d1, 0, h, fsdp_gains[1, 1:], "down_full")
        y = lax.all_gather(y, 'tp', axis=0, tiled=False)

        def cache(first, second):
            return jnp.stack([first, second.reshape(shape3)]).reshape(2, batch, seq_len, part // HEAD_DIM, HEAD_DIM)

        return y, cache(keys_rot, k_heads), cache(values, v_heads)

    return jax.shard_map(local_layers, mesh=mesh,
                         in_specs=(act_spec, in_cols, in_cols, in_cols, in_rows, in_cols, in_cols, in_rows,
                                   tp_gain, tp_gain, fsdp_gain, fsdp_gain),
                         out_specs=(act_spec, cache_spec, cache_spec), check_vma=False)
```

```python
import jax
import jax.numpy as jnp
from jax import lax
from jax.experimental import pallas as pl
from jax.experimental.pallas import tpu as pltpu
from jax.sharding import PartitionSpec as P


HEAD_DIM = 128
NORM_EPS = 1e-6
ROPE_THETA = 500000.0
CHUNKS = 2
QB = 256
F32, BF16 = jnp.float32, jnp.bfloat16


def rope_tables(seq_len):
    half = HEAD_DIM // 2
    inv_freq = ROPE_THETA ** (-2.0 * jnp.arange(half, dtype=F32) / HEAD_DIM)
    angles = jnp.arange(seq_len, dtype=F32)[:, None] * inv_freq[None, :]
    cos_t, sin_t = jnp.cos(angles), jnp.sin(angles)
    return jnp.concatenate([cos_t, cos_t], axis=-1), jnp.concatenate([-sin_t, sin_t], axis=-1)


def dot(a, b):
    return jnp.dot(a, b, preferred_element_type=F32)


def params(*semantics):
    return pltpu.CompilerParams(dimension_semantics=semantics or ("arbitrary",), vmem_limit_bytes=60 * 1024 * 1024)


def cost(flops, nbytes):
    return pl.CostEstimate(flops=flops, bytes_accessed=nbytes, transcendentals=0)


def rotate(vals, cos_t, sin_t):
    return vals * cos_t + pltpu.roll(vals, HEAD_DIM // 2, 1) * sin_t


def qkv_raw(x, w):
    tokens, width = x.shape
    part = w.shape[1] // 3
    tm = min(512, tokens)

    def body(x_ref, w_ref, q_ref, k_ref, v_ref, sq_ref):
        xb = x_ref[...]
        q = dot(xb, w_ref[:, :part])
        q_ref[...] = q
        q_sq = jnp.sum(q * q, axis=-1, keepdims=True)
        k = dot(xb, w_ref[:, part:2 * part])
        k_ref[...] = k
        k_sq = jnp.sum(k * k, axis=-1, keepdims=True)
        v_ref[...] = dot(xb, w_ref[:, 2 * part:]).astype(BF16)
        lane = lax.broadcasted_iota(jnp.int32, (tm, 128), 1)
        cols = jnp.where(lane == 0, q_sq, jnp.where(lane == 1, k_sq, 0.0))
        sq_ref[...] = cols.T[:8, :]

    row = lambda i: (i, 0)
    return pl.pallas_call(
        body, grid=(tokens // tm,),
        in_specs=[pl.BlockSpec((tm, width), row), pl.BlockSpec(w.shape, lambda i: (0, 0), pipeline_mode=pl.Buffered(1))],
        out_specs=[pl.BlockSpec((tm, part), row)] * 3 + [pl.BlockSpec((8, tm), lambda i: (0, i))],
        out_shape=[jax.ShapeDtypeStruct((tokens, part), d) for d in (F32, F32, BF16)]
        + [jax.ShapeDtypeStruct((8, tokens), F32)],
        compiler_params=params(), cost_estimate=cost(2 * tokens * width * 3 * part, 2 * tokens * width + 10 * tokens * part),
        name="qkv_raw")(x, w)


def norm_rope(q_raw, k_raw, inv, q_gain, k_gain, cos_t, sin_t):
    tokens, part = q_raw.shape
    tm = min(512, cos_t.shape[0])
    per_seq = cos_t.shape[0] // tm

    def body(q_ref, k_ref, inv_ref, qg_ref, kg_ref, cos_ref, sin_ref, qo_ref, ko_ref):
        for n, (src, gain, dst) in enumerate(((q_ref, qg_ref, qo_ref), (k_ref, kg_ref, ko_ref))):
            scale = jnp.broadcast_to(inv_ref[n:n + 1, :], (128, tm)).T
            for h in range(part // HEAD_DIM):
                cols = slice(h * HEAD_DIM, (h + 1) * HEAD_DIM)
                vals = src[:, cols] * scale * gain[:, cols]
                dst[:, cols] = rotate(vals, cos_ref[...], sin_ref[...]).astype(BF16)

    row = lambda i: (i, 0)
    gain = pl.BlockSpec((1, part), lambda i: (0, 0))
    table = pl.BlockSpec((tm, HEAD_DIM), lambda i: (lax.rem(i, per_seq), 0))
    return pl.pallas_call(
        body, grid=(tokens // tm,),
        in_specs=[pl.BlockSpec((tm, part), row)] * 2 + [pl.BlockSpec((8, tm), lambda i: (0, i)), gain, gain, table, table],
        out_specs=[pl.BlockSpec((tm, part), row)] * 2,
        out_shape=[jax.ShapeDtypeStruct((tokens, part), BF16)] * 2,
        compiler_params=params(), cost_estimate=cost(tokens * part * 2000, tokens * part * 12),
        name="norm_rope")(q_raw, k_raw, inv, q_gain, k_gain, cos_t, sin_t)


def softmax_pv(q, past, k, v):
    rows = q.shape[0]
    nt = (((1,), (1,)), ((), ()))
    scale = HEAD_DIM ** -0.5
    diag = lax.dot_general(q, k, nt, preferred_element_type=F32) * scale
    keep = lax.broadcasted_iota(jnp.int32, (rows, rows), 0) >= lax.broadcasted_iota(jnp.int32, (rows, rows), 1)
    diag = jnp.where(keep, diag, -jnp.inf)
    top = jnp.max(diag, axis=-1, keepdims=True)
    scores = [(lax.dot_general(q, pk, nt, preferred_element_type=F32) * scale, pv) for pk, pv in past]
    for left, _ in scores:
        top = jnp.maximum(top, jnp.max(left, axis=-1, keepdims=True))
    probs = [(jnp.exp(left - top), pv) for left, pv in scores] + [(jnp.exp(diag - top), v)]
    total = sum(jnp.sum(p, axis=-1, keepdims=True) for p, _ in probs)
    inv = 1.0 / total
    out = sum(dot((p * inv).astype(BF16), pv) for p, pv in probs)
    return out.astype(BF16)


def attention(q, q_block, qc, kvs):
    seqs, _, group = q.shape
    qb = min(QB, qc)
    heads = group // HEAD_DIM
    half = group // 2
    own = kvs[-1][2] - qc

    def body(q_ref, *refs):
        k_refs, v_refs, (a_ref, b_ref) = refs[:len(kvs)], refs[len(kvs):2 * len(kvs)], refs[2 * len(kvs):]
        for h in range(heads):
            cols = slice(h * HEAD_DIM, (h + 1) * HEAD_DIM)
            dst = (a_ref, b_ref)[h * HEAD_DIM // half]
            dcols = slice(h * HEAD_DIM % half, h * HEAD_DIM % half + HEAD_DIM)
            for j in range(qc // qb):
                first = own + j * qb
                past = [(k_refs[n][0, :, cols], v_refs[n][0, :, cols]) for n in range(len(kvs) - 1)]
                if first:
                    past.append((k_refs[-1][0, :first, cols], v_refs[-1][0, :first, cols]))
                dst[0, j * qb:(j + 1) * qb, dcols] = softmax_pv(
                    q_ref[0, j * qb:(j + 1) * qb, cols], past,
                    k_refs[-1][0, first:first + qb, cols], v_refs[-1][0, first:first + qb, cols])

    kv = [pl.BlockSpec((1, rows, group), lambda s: (s, 0, 0)) for _, _, rows in kvs]
    keys = sum(rows for _, _, rows in kvs)
    out = pl.BlockSpec((1, qc, half), lambda s: (s, 0, 0))
    return pl.pallas_call(
        body, grid=(seqs,),
        in_specs=[pl.BlockSpec((1, qc, group), lambda s: (s, q_block, 0))] + kv + kv,
        out_specs=[out, out],
        out_shape=[jax.ShapeDtypeStruct((seqs, qc, half), BF16)] * 2,
        compiler_params=params(),
        cost_estimate=cost(8 * seqs * qc * keys * group, seqs * group * 2 * (2 * qc + 2 * keys)))(q, *(k for k, _, _ in kvs), *(v for _, v, _ in kvs))


def out_proj_gathered(order, outs, w, x, gain, chunk):
    seqs, qc, half = outs[0].shape
    width = x.shape[2]
    shards, sources, _, cols = w.shape

    def body(order_ref, *refs):
        o_refs, (w_ref, x_ref, gain_ref, ha_ref, hb_ref, a_ref) = refs[:2 * sources], refs[2 * sources:]
        sq = jnp.zeros((qc, 1), F32)
        for f in range(shards):
            acc = jnp.zeros((qc, cols), F32)
            for s in range(sources):
                src = order_ref[s]
                acc += dot(o_refs[2 * s][0], w_ref[f, src, :half, :])
                acc += dot(o_refs[2 * s + 1][0], w_ref[f, src, half:, :])
            a = acc.astype(BF16)
            a_ref[:, f * cols:(f + 1) * cols] = a
            a = a.astype(F32)
            sq += jnp.sum(a * a, axis=-1, keepdims=True)
        inv = lax.rsqrt(sq / width + NORM_EPS)
        for f in range(shards):
            c = slice(f * cols, (f + 1) * cols)
            h_ref = (ha_ref, hb_ref)[f // (shards // 2)]
            hc = slice(f % (shards // 2) * cols, (f % (shards // 2) + 1) * cols)
            h_ref[0, :, hc] = (x_ref[0, :, c].astype(F32) + a_ref[:, c].astype(F32) * inv * gain_ref[:, c]).astype(BF16)

    o_spec = pl.BlockSpec((1, qc, half), lambda r, order: (order[r], 0, 0))
    return pl.pallas_call(
        body,
        grid_spec=pltpu.PrefetchScalarGridSpec(
            num_scalar_prefetch=1, grid=(seqs,),
            in_specs=[o_spec] * (2 * sources) + [
                pl.BlockSpec(w.shape, lambda r, order: (0, 0, 0, 0), pipeline_mode=pl.Buffered(1)),
                pl.BlockSpec((1, qc, width), lambda r, order: (order[r], chunk, 0)),
                pl.BlockSpec((1, width), lambda r, order: (0, 0))],
            out_specs=[pl.BlockSpec((1, qc, width // 2), lambda r, order: (r, 0, 0))] * 2,
            scratch_shapes=[pltpu.VMEM((qc, width), BF16)]),
        out_shape=[jax.ShapeDtypeStruct((seqs, qc, width // 2), BF16)] * 2,
        compiler_params=params(), cost_estimate=cost(2 * seqs * qc * width * width, 6 * seqs * qc * width + 2 * width * width))(order, *outs, w, x, gain)


def mlp_up(hs, w, gate_spec, up_spec, first, steps):
    seqs = len(hs)
    qc, half = hs[0][0].shape
    width = 2 * half
    tn = 256

    def body(*refs):
        h_refs, (g_ref, u_ref, act_ref) = refs[:2 * seqs], refs[2 * seqs:]
        g = g_ref[...].reshape(width, tn)
        u = u_ref[...].reshape(width, tn)
        for s in range(seqs):
            ha, hb = h_refs[2 * s][...], h_refs[2 * s + 1][...]
            gate = dot(ha, g[:half]) + dot(hb, g[half:])
            up = dot(ha, u[:half]) + dot(hb, u[half:])
            act_ref[s * qc:(s + 1) * qc, :] = (jax.nn.silu(gate) * up).astype(BF16)

    index = lambda i: first + i
    fixed = pl.BlockSpec((qc, half), lambda i: (0, 0), pipeline_mode=pl.Buffered(1))
    rows = seqs * qc
    flat = [a for pair in hs for a in pair]
    return pl.pallas_call(
        body, grid=(steps,),
        in_specs=[fixed] * (2 * seqs) + [gate_spec(index), up_spec(index)],
        out_specs=pl.BlockSpec((rows, tn), lambda i: (0, i)),
        out_shape=jax.ShapeDtypeStruct((rows, steps * tn), BF16),
        compiler_params=params(), cost_estimate=cost(4 * rows * width * steps * tn, 2 * rows * width + 4 * width * steps * tn))(*flat, w, w)


def mlp_down(acts, w, down_spec, seqs, width):
    rows = acts[0].shape[0]
    qc = rows // seqs
    ff = sum(a.shape[1] for a in acts)
    n = len(acts)
    tn = 256
    half = width // 2
    per_side = half // tn

    def body(*refs):
        act_refs, d_ref, outs = refs[:n], refs[n], refs[n + 1:]
        d = d_ref[...].reshape(ff, tn)
        step = pl.program_id(0)

        def product(s):
            acc = jnp.zeros((qc, tn), F32)
            at = 0
            for a in act_refs:
                acc += dot(a[s * qc:(s + 1) * qc, :], d[at:at + a.shape[1]])
                at += a.shape[1]
            return acc.astype(BF16)

        for side in range(2):
            @pl.when(step // per_side == side)
            def _(side=side):
                for s in range(seqs):
                    outs[2 * s + side][...] = product(s)

    first = pl.BlockSpec((qc, tn), lambda i: (0, jnp.minimum(i, per_side - 1)))
    second = pl.BlockSpec((qc, tn), lambda i: (0, jnp.maximum(i - per_side, 0)))
    return pl.pallas_call(
        body, grid=(2 * per_side,),
        in_specs=[pl.BlockSpec(a.shape, lambda i: (0, 0), pipeline_mode=pl.Buffered(1)) for a in acts] + [down_spec(lambda i: i)],
        out_specs=[first, second] * seqs,
        out_shape=[jax.ShapeDtypeStruct((qc, half), BF16)] * (2 * seqs),
        compiler_params=params(), cost_estimate=cost(2 * rows * width * ff, 2 * rows * (width + ff) + 2 * width * ff))(*acts, w)


def finish(parts_a, parts_b, h_a, h_b, gain, place, whole):
    rows, half = h_a.shape
    width = 2 * half
    block = 256
    per_side = half // block
    tr = min(256, rows)
    n = len(parts_a)

    def body(*refs):
        pa, pb = refs[:n], refs[n:2 * n]
        h_refs, gain_ref, outs = refs[2 * n:2 * n + 2], refs[2 * n + 2], refs[2 * n + 3:]
        sums = []
        for side in (pa, pb):
            m = side[0][...].astype(F32)
            for p in side[1:]:
                m = m + p[...].astype(F32)
            sums.append(m.astype(BF16).astype(F32))
        sq = sum(jnp.sum(m * m, axis=-1, keepdims=True) for m in sums)
        inv = lax.rsqrt(sq / width + NORM_EPS)
        for side in range(2):
            for b in range(per_side):
                c = slice(b * block, (b + 1) * block)
                at = place(side, b)
                gain_cols = gain_ref[:, at * block:(at + 1) * block]
                val = (h_refs[side][:, c].astype(F32) + sums[side][:, c] * inv * gain_cols).astype(BF16)
                if whole:
                    outs[0][:, at * block:(at + 1) * block] = val
                else:
                    at_half = at % per_side
                    outs[at // per_side][:, at_half * block:(at_half + 1) * block] = val

    part = pl.BlockSpec((tr, half), lambda i: (i, 0))
    out_width = width if whole else half
    outs = 1 if whole else 2
    return pl.pallas_call(
        body, grid=(rows // tr,),
        in_specs=[part] * (2 * n + 2) + [pl.BlockSpec((1, width), lambda i: (0, 0))],
        out_specs=[pl.BlockSpec((tr, out_width), lambda i: (i, 0))] * outs,
        out_shape=[jax.ShapeDtypeStruct((rows, out_width), BF16)] * outs,
        compiler_params=params(), cost_estimate=cost(rows * width * 2000, rows * width * 2 * (n + 2)))(*parts_a, *parts_b, h_a, h_b, gain)


def qkv_full(x, w, q_gain, k_gain, cos_t, sin_t, part, chunk):
    tokens, width = x.shape
    shards, tps, _, cols = w.shape
    depth = width // shards
    per = part // cols
    blocks = tps * per
    tr = min(256, tokens)

    def body(x_ref, w_ref, qg_ref, kg_ref, cos_ref, sin_ref, q_ref, k_ref, v_ref, raw_ref, sq_ref):
        which, n = pl.program_id(0), pl.program_id(1)
        out = dot(x_ref[...], w_ref[...].reshape(width, cols))

        @pl.when(which < 2)
        def _():
            raw_ref[n] = out
            part_sq = jnp.sum(out * out, axis=-1, keepdims=True)
            sq_ref[...] = jnp.where(n == 0, 0.0, sq_ref[...]) + part_sq

        @pl.when(which == 2)
        def _():
            v_ref[0] = out.astype(BF16)

        for sel, (gain, dst) in enumerate(((qg_ref, q_ref), (kg_ref, k_ref))):
            @pl.when((which == sel) & (n == blocks - 1))
            def _(gain=gain, dst=dst):
                def rows_body(r, _):
                    rows = pl.ds(r * tr, tr)
                    inv = lax.rsqrt(sq_ref[rows, :] / width + NORM_EPS)
                    for m in range(blocks):
                        for h in range(cols // HEAD_DIM):
                            lanes = slice(h * HEAD_DIM, (h + 1) * HEAD_DIM)
                            wide = slice(m * cols + h * HEAD_DIM, m * cols + (h + 1) * HEAD_DIM)
                            deep = slice(m % per * cols + h * HEAD_DIM, m % per * cols + (h + 1) * HEAD_DIM)
                            vals = raw_ref[m, rows, lanes] * inv * gain[:, wide]
                            dst[m // per, rows, deep] = rotate(vals, cos_ref[rows, :], sin_ref[rows, :]).astype(BF16)
                    return 0

                lax.fori_loop(0, tokens // tr, rows_body, 0)

    fixed = lambda s: pl.BlockSpec(s, lambda i, n: (0,) * len(s), pipeline_mode=pl.Buffered(1))
    whole = pl.BlockSpec((tps, tokens, part), lambda i, n: (0, 0, 0))
    table = pl.BlockSpec((tokens, HEAD_DIM), lambda i, n: (chunk, 0), pipeline_mode=pl.Buffered(1))
    return pl.pallas_call(
        body, grid=(3, blocks),
        in_specs=[fixed((tokens, width)),
                  pl.BlockSpec((shards, 1, depth, cols), lambda i, n: (0, n // per, i * per + n % per, 0)),
                  fixed((1, width)), fixed((1, width)), table, table],
        out_specs=[whole, whole, pl.BlockSpec((1, tokens, cols), lambda i, n: (jnp.where(i == 2, n // per, 0), 0, jnp.where(i == 2, n % per, 0)))],
        out_shape=[jax.ShapeDtypeStruct((tps, tokens, part), BF16)] * 3,
        scratch_shapes=[pltpu.VMEM((blocks, tokens, cols), F32), pltpu.VMEM((tokens, 1), F32)],
        compiler_params=params("arbitrary", "arbitrary"),
        cost_estimate=cost(6 * tokens * width * width, 8 * tokens * width + 6 * width * width))(x, w, q_gain, k_gain, cos_t, sin_t)


def out_proj_full(o_a, o_b, w, row_block, depth, x, gain):
    tokens, width = x.shape
    shards, tps, _, cols = w.shape
    half = depth // 2
    tr = min(256, tokens)

    def body(oa_ref, ob_ref, w_ref, x_ref, gain_ref, ha_ref, hb_ref, o_ref, raw_ref, sq_ref):
        f = pl.program_id(0)

        @pl.when(f == 0)
        def _():
            for t in range(tps):
                o_ref[:, t * depth:t * depth + half] = oa_ref[t]
                o_ref[:, t * depth + half:(t + 1) * depth] = ob_ref[t]

        out = dot(o_ref[...], w_ref[...].reshape(tps * depth, cols)).astype(BF16)
        raw_ref[f] = out
        out = out.astype(F32)
        sq_ref[...] = jnp.where(f == 0, 0.0, sq_ref[...]) + jnp.sum(out * out, axis=-1, keepdims=True)

        @pl.when(f == shards - 1)
        def _():
            def rows_body(r, _):
                rows = pl.ds(r * tr, tr)
                inv = lax.rsqrt(sq_ref[rows, :] / width + NORM_EPS)
                for m in range(shards):
                    c = slice(m * cols, (m + 1) * cols)
                    dst = slice(m // 2 * cols, (m // 2 + 1) * cols)
                    (ha_ref, hb_ref)[m % 2][rows, dst] = (
                        x_ref[rows, c].astype(F32) + raw_ref[m, rows, :].astype(F32) * inv * gain_ref[:, c]).astype(BF16)
                return 0

            lax.fori_loop(0, tokens // tr, rows_body, 0)

    fixed = lambda s: pl.BlockSpec(s, lambda f: (0,) * len(s), pipeline_mode=pl.Buffered(1))
    return pl.pallas_call(
        body, grid=(shards,),
        in_specs=[fixed(o_a.shape), fixed(o_b.shape), pl.BlockSpec((1, tps, depth, cols), lambda f: (f, 0, row_block, 0)),
                  fixed((tokens, width)), fixed((1, width))],
        out_specs=[pl.BlockSpec((tokens, width // 2), lambda f: (0, 0))] * 2,
        out_shape=[jax.ShapeDtypeStruct((tokens, width // 2), BF16)] * 2,
        scratch_shapes=[pltpu.VMEM((tokens, width), BF16), pltpu.VMEM((shards, tokens, cols), BF16), pltpu.VMEM((tokens, 1), F32)],
        compiler_params=params(),
        cost_estimate=cost(2 * tokens * width * width, 2 * width * (width + 2 * tokens)))(o_a, o_b, w, x, gain)


class Ring:
    def __init__(self, axis, size):
        assert size == 4
        self.axis, self.size = axis, size

    def up(self, a):
        return lax.ppermute(a, self.axis, [(i, (i + 1) % self.size) for i in range(self.size)])

    def down(self, a):
        return lax.ppermute(a, self.axis, [(i, (i - 1) % self.size) for i in range(self.size)])

    def gather(self, a, b):
        below_a, above_b = self.up(a), self.down(b)
        below_b, above_a = self.up(b), self.down(a)
        far_a, far_b = self.up(below_a), self.down(above_b)
        return [(a, b), (above_a, above_b), (far_a, far_b), (below_a, below_b)]

    def scatter(self, parts):
        own_a, own_b, one_a, one_b, two_a, two_b, three_a, three_b = parts
        far_a, far_b = self.up(two_a), self.down(two_b)
        below_b, above_a = self.up(one_b), self.down(three_a)
        below_a = self.up(one_a + far_a)
        above_b = self.down(three_b + far_b)
        return [own_a, below_a, above_a], [own_b, below_b, above_b]


def solution(mesh):
    cores = 2
    dp, tp, fsdp = mesh.shape['dp'], mesh.shape['tp'], mesh.shape['fsdp']
    xs = fsdp // cores
    mesh = jax.sharding.Mesh(mesh.devices.reshape(dp, tp, xs, cores), ('dp', 'tp', 'x', 'c'))
    shards = ('x', 'c')
    batch_axes = ('dp', 'x', 'c')
    act_spec = P(batch_axes, None, None)
    in_cols = P(None, shards, 'tp')
    in_rows = P(None, 'tp', shards)
    tp_gain = P(None, 'tp')
    fsdp_gain = P(None, shards)
    cache_spec = P(None, batch_axes, None, 'tp', None)
    ring_y, ring_x = Ring('tp', tp), Ring('x', xs)

    def gather_all(a):
        g = lax.all_gather(a, ('x', 'c', 'tp'), axis=0, tiled=False)
        return g.reshape(fsdp, tp, *a.shape)

    def blocks_of(w, cols):
        return [w[:, i:i + cols] for i in range(0, w.shape[1], cols)]

    def local_layers(x, w_query, w_key, w_value, w_out, w_gate, w_up, w_down, q_norm_w, k_norm_w, attn_norm_w, ffn_norm_w):
        batch, seq_len, width = x.shape
        assert batch == tp and w_query.shape[0] == 2
        tokens = batch * seq_len
        qc = seq_len // CHUNKS
        part = w_query.shape[2]
        cols = w_out.shape[2]
        ff = w_gate.shape[2]
        per_side = width // 2 // cols
        cos_t, sin_t = rope_tables(seq_len)
        me = lax.axis_index('tp')
        seq_order = lax.rem(me + jnp.arange(tp, dtype=jnp.int32), tp)

        w_qkv = lax.all_gather(jnp.concatenate([w_query[0], w_key[0], w_value[0]], axis=1), shards, axis=0, tiled=True)
        fsdp_gains = lax.all_gather(jnp.stack([attn_norm_w, ffn_norm_w]), shards, axis=2, tiled=True)
        tp_gains = lax.all_gather(jnp.stack([q_norm_w[1], k_norm_w[1]]), 'tp', axis=1, tiled=True)
        x, fsdp_gains, tp_gains = lax.optimization_barrier((x, fsdp_gains, tp_gains))
        w_o0 = gather_all(w_out[0])
        w_gu0 = lax.all_gather(jnp.concatenate([w_gate[0], w_up[0]], axis=1), shards, axis=0, tiled=True)
        w_d0 = lax.all_gather(w_down[0], shards, axis=0, tiled=False)
        w_attn1 = gather_all(jnp.concatenate(
            blocks_of(w_query[1], cols) + blocks_of(w_key[1], cols) + blocks_of(w_value[1], cols) + [w_out[1]], axis=0))
        share = ff // xs
        pieces = [jnp.concatenate(blocks_of(w_gate[1][:, i * share:(i + 1) * share], cols)
                                  + blocks_of(w_up[1][:, i * share:(i + 1) * share], cols)
                                  + [w_down[1][i * share:(i + 1) * share]], axis=0) for i in range(xs)]
        mlp1 = lax.all_to_all(jnp.stack(pieces), 'x', split_axis=0, concat_axis=0, tiled=True)
        mlp1 = lax.all_gather(mlp1, ('c', 'tp'), axis=0, tiled=False)
        mlp1 = mlp1.reshape(cores, tp, *mlp1.shape[1:])
        depth = w_gate.shape[1]
        up_rows = share // cols * depth

        q_raw, k_raw, values, sq = qkv_raw(x.reshape(tokens, width), w_qkv)
        sq_up, sq_down = ring_y.up(sq), ring_y.down(sq)
        sq_far = lax.ppermute(sq, 'tp', [(i, (i + 2) % tp) for i in range(tp)])
        inv = lax.rsqrt((sq + sq_up + sq_down + sq_far) / width + NORM_EPS)
        queries, keys_rot = norm_rope(q_raw, k_raw, inv, q_norm_w[:1], k_norm_w[:1], cos_t, sin_t)
        shape3 = (batch, seq_len, part)
        queries, keys_rot, values = (a.reshape(shape3) for a in (queries, keys_rot, values))

        def mlp(hs, w, gate, up, w_down, down, ff):
            steps = ff // 256 // 2
            acts = [mlp_up(hs, w, gate, up, i * steps, steps) for i in range(2)]
            return mlp_down(acts, w_down, down, len(hs), width)

        def cols_spec(offset):
            return lambda index: pl.BlockSpec((width, 256), lambda i: (0, offset + index(i)))

        gate0, up0 = cols_spec(0), cols_spec(ff // 256)
        down0 = lambda index: pl.BlockSpec((1, ff, cols), lambda i: (index(i), 0, 0))
        gathered = []
        for c in range(CHUNKS):
            own = attention(queries, c, qc, [(keys_rot, values, qc * (c + 1))])
            gathered.append(ring_y.gather(*own))
        sums, own_h = [], []
        for c in range(CHUNKS):
            outs = [a for pair in gathered[c] for a in pair]
            h_a, h_b = out_proj_gathered(seq_order, outs, w_o0, x, fsdp_gains[0, :1], c)
            sums.append(mlp([(h_a[s], h_b[s]) for s in range(batch)], w_gu0, gate0, up0, w_d0, down0, ff))
            own_h.append((h_a[0], h_b[0]))

        def up_spec(block):
            return lambda index: pl.BlockSpec((cores, 1, xs, depth, 256),
                                              lambda i: (0, index(i) // (share // 256), 0, block + index(i) % (share // 256), 0))

        gate1, up1 = up_spec(0), up_spec(share // 256)
        down1 = lambda index: pl.BlockSpec((1, tp, 1, share, cols), lambda i: (index(i) // xs, 0, index(i) % xs, 2 * up_rows // share, 0))
        kvs, caches, h1, gathered = [], [], [], []
        for c in range(CHUNKS):
            sum_a, sum_b = ring_y.scatter(sums[c])
            hidden, = finish(sum_a, sum_b, *own_h[c], fsdp_gains[1, :1], lambda side, b: side * per_side + b, True)
            q1, k1, v1 = qkv_full(hidden, w_attn1, tp_gains[:1], tp_gains[1:], cos_t, sin_t, part, c)
            caches.append([lax.all_to_all(a, 'tp', split_axis=0, concat_axis=0, tiled=True) for a in (k1, v1)])
            kvs.append((k1, v1, qc))
            own = attention(q1, 0, qc, list(kvs))
            h1.append(out_proj_full(*own, w_attn1, 3 * part * depth // cols // w_out.shape[1], w_out.shape[1], hidden,
                                    fsdp_gains[0, 1:]))
            gathered.append(ring_x.gather(*h1[-1]))
        sums = []
        for c in range(CHUNKS):
            hs = gathered[c]
            if c == CHUNKS - 1:
                hs, caches = lax.optimization_barrier((hs, caches))
            sums.append(mlp(hs, mlp1, gate1, up1, mlp1, down1, tp * share))
        y = jnp.zeros(x.shape, BF16)
        for c in range(CHUNKS):
            sum_a, sum_b = ring_x.scatter(sums[c])
            y_own = finish(sum_a, sum_b, *h1[c], fsdp_gains[1, 1:], lambda side, b: 2 * b + side, False)
            for rel, pair in enumerate(ring_y.gather(*y_own)):
                for side in range(2):
                    y = lax.dynamic_update_slice(y, pair[side][None], (seq_order[rel], c * qc, side * width // 2))

        def cache(first, n):
            second = jnp.concatenate([caches[c][n] for c in range(CHUNKS)], axis=1)
            return jnp.stack([first, second]).reshape(2, batch, seq_len, part // HEAD_DIM, HEAD_DIM)

        return y, cache(keys_rot, 0), cache(values, 1)

    return jax.shard_map(local_layers, mesh=mesh,
                         in_specs=(act_spec, in_cols, in_cols, in_cols, in_rows, in_cols, in_cols, in_rows,
                                   tp_gain, tp_gain, fsdp_gain, fsdp_gain),
                         out_specs=(act_spec, cache_spec, cache_spec), check_vma=False)
```

```python
import jax
import jax.numpy as jnp
from jax import lax
from jax.experimental import pallas as pl
from jax.experimental.pallas import tpu as pltpu
from jax.sharding import PartitionSpec as P


HEAD_DIM = 128
NORM_EPS = 1e-6
ROPE_THETA = 500000.0
CHUNKS = 2
QB = 256
F32, BF16 = jnp.float32, jnp.bfloat16


def rope_tables(seq_len):
    half = HEAD_DIM // 2
    inv_freq = ROPE_THETA ** (-2.0 * jnp.arange(half, dtype=F32) / HEAD_DIM)
    angles = jnp.arange(seq_len, dtype=F32)[:, None] * inv_freq[None, :]
    cos_t, sin_t = jnp.cos(angles), jnp.sin(angles)
    return jnp.concatenate([cos_t, cos_t], axis=-1), jnp.concatenate([-sin_t, sin_t], axis=-1)


def dot(a, b):
    return jnp.dot(a, b, preferred_element_type=F32)


def params(*semantics):
    return pltpu.CompilerParams(dimension_semantics=semantics or ("arbitrary",), vmem_limit_bytes=60 * 1024 * 1024)


def cost(flops, nbytes):
    return pl.CostEstimate(flops=flops, bytes_accessed=nbytes, transcendentals=0)


def rotate(vals, cos_t, sin_t):
    return vals * cos_t + pltpu.roll(vals, HEAD_DIM // 2, 1) * sin_t


def qkv_raw(x, w):
    tokens, width = x.shape
    part = w.shape[1] // 3
    tm = min(512, tokens)

    def body(x_ref, w_ref, q_ref, k_ref, v_ref, sq_ref):
        xb = x_ref[...]
        q = dot(xb, w_ref[:, :part])
        q_ref[...] = q
        q_sq = jnp.sum(q * q, axis=-1, keepdims=True)
        k = dot(xb, w_ref[:, part:2 * part])
        k_ref[...] = k
        k_sq = jnp.sum(k * k, axis=-1, keepdims=True)
        v_ref[...] = dot(xb, w_ref[:, 2 * part:]).astype(BF16)
        lane = lax.broadcasted_iota(jnp.int32, (tm, 128), 1)
        cols = jnp.where(lane == 0, q_sq, jnp.where(lane == 1, k_sq, 0.0))
        sq_ref[...] = cols.T[:8, :]

    row = lambda i: (i, 0)
    return pl.pallas_call(
        body, grid=(tokens // tm,),
        in_specs=[pl.BlockSpec((tm, width), row), pl.BlockSpec(w.shape, lambda i: (0, 0), pipeline_mode=pl.Buffered(1))],
        out_specs=[pl.BlockSpec((tm, part), row)] * 3 + [pl.BlockSpec((8, tm), lambda i: (0, i))],
        out_shape=[jax.ShapeDtypeStruct((tokens, part), d) for d in (F32, F32, BF16)]
        + [jax.ShapeDtypeStruct((8, tokens), F32)],
        compiler_params=params(), cost_estimate=cost(2 * tokens * width * 3 * part, 2 * tokens * width + 10 * tokens * part),
        name="qkv_raw")(x, w)


def norm_rope(q_raw, k_raw, inv, q_gain, k_gain, cos_t, sin_t):
    tokens, part = q_raw.shape
    tm = min(512, cos_t.shape[0])
    per_seq = cos_t.shape[0] // tm

    def body(q_ref, k_ref, inv_ref, qg_ref, kg_ref, cos_ref, sin_ref, qo_ref, ko_ref):
        for n, (src, gain, dst) in enumerate(((q_ref, qg_ref, qo_ref), (k_ref, kg_ref, ko_ref))):
            scale = jnp.broadcast_to(inv_ref[n:n + 1, :], (128, tm)).T
            for h in range(part // HEAD_DIM):
                cols = slice(h * HEAD_DIM, (h + 1) * HEAD_DIM)
                vals = src[:, cols] * scale * gain[:, cols]
                dst[:, cols] = rotate(vals, cos_ref[...], sin_ref[...]).astype(BF16)

    row = lambda i: (i, 0)
    gain = pl.BlockSpec((1, part), lambda i: (0, 0))
    table = pl.BlockSpec((tm, HEAD_DIM), lambda i: (lax.rem(i, per_seq), 0))
    return pl.pallas_call(
        body, grid=(tokens // tm,),
        in_specs=[pl.BlockSpec((tm, part), row)] * 2 + [pl.BlockSpec((8, tm), lambda i: (0, i)), gain, gain, table, table],
        out_specs=[pl.BlockSpec((tm, part), row)] * 2,
        out_shape=[jax.ShapeDtypeStruct((tokens, part), BF16)] * 2,
        compiler_params=params(), cost_estimate=cost(tokens * part * 2000, tokens * part * 12),
        name="norm_rope")(q_raw, k_raw, inv, q_gain, k_gain, cos_t, sin_t)


def softmax_pv(q, past, k, v):
    rows = q.shape[0]
    nt = (((1,), (1,)), ((), ()))
    scale = HEAD_DIM ** -0.5
    diag = lax.dot_general(q, k, nt, preferred_element_type=F32) * scale
    keep = lax.broadcasted_iota(jnp.int32, (rows, rows), 0) >= lax.broadcasted_iota(jnp.int32, (rows, rows), 1)
    diag = jnp.where(keep, diag, -jnp.inf)
    top = jnp.max(diag, axis=-1, keepdims=True)
    scores = [(lax.dot_general(q, pk, nt, preferred_element_type=F32) * scale, pv) for pk, pv in past]
    for left, _ in scores:
        top = jnp.maximum(top, jnp.max(left, axis=-1, keepdims=True))
    probs = [(jnp.exp(left - top), pv) for left, pv in scores] + [(jnp.exp(diag - top), v)]
    total = sum(jnp.sum(p, axis=-1, keepdims=True) for p, _ in probs)
    inv = 1.0 / total
    out = sum(dot((p * inv).astype(BF16), pv) for p, pv in probs)
    return out.astype(BF16)


def attention(q, q_block, qc, kvs):
    seqs, _, group = q.shape
    qb = min(QB, qc)
    heads = group // HEAD_DIM
    half = group // 2
    own = kvs[-1][2] - qc

    def body(q_ref, *refs):
        k_refs, v_refs, (a_ref, b_ref) = refs[:len(kvs)], refs[len(kvs):2 * len(kvs)], refs[2 * len(kvs):]
        for h in range(heads):
            cols = slice(h * HEAD_DIM, (h + 1) * HEAD_DIM)
            dst = (a_ref, b_ref)[h * HEAD_DIM // half]
            dcols = slice(h * HEAD_DIM % half, h * HEAD_DIM % half + HEAD_DIM)
            for j in range(qc // qb):
                first = own + j * qb
                past = [(k_refs[n][0, :, cols], v_refs[n][0, :, cols]) for n in range(len(kvs) - 1)]
                if first:
                    past.append((k_refs[-1][0, :first, cols], v_refs[-1][0, :first, cols]))
                dst[0, j * qb:(j + 1) * qb, dcols] = softmax_pv(
                    q_ref[0, j * qb:(j + 1) * qb, cols], past,
                    k_refs[-1][0, first:first + qb, cols], v_refs[-1][0, first:first + qb, cols])

    kv = [pl.BlockSpec((1, rows, group), lambda s: (s, 0, 0)) for _, _, rows in kvs]
    keys = sum(rows for _, _, rows in kvs)
    out = pl.BlockSpec((1, qc, half), lambda s: (s, 0, 0))
    return pl.pallas_call(
        body, grid=(seqs,),
        in_specs=[pl.BlockSpec((1, qc, group), lambda s: (s, q_block, 0))] + kv + kv,
        out_specs=[out, out],
        out_shape=[jax.ShapeDtypeStruct((seqs, qc, half), BF16)] * 2,
        compiler_params=params(),
        cost_estimate=cost(8 * seqs * qc * keys * group, seqs * group * 2 * (2 * qc + 2 * keys)))(q, *(k for k, _, _ in kvs), *(v for _, v, _ in kvs))


def out_proj_gathered(order, outs, w, x, gain, chunk):
    seqs, qc, half = outs[0].shape
    width = x.shape[2]
    shards, sources, _, cols = w.shape
    depth = 2 * half
    group = 2
    rows = group * qc

    def body(order_ref, *refs):
        o_refs, (w_ref, x0_ref, x1_ref, gain_ref, ha_ref, hb_ref, o_ref, a_ref, sems) = refs[:2 * sources], refs[2 * sources:]
        step = pl.program_id(0)

        def copies(g):
            for j in range(group):
                for s in range(sources):
                    for side in range(2):
                        at = pl.multiple_of(order_ref[s] * depth + side * half, half)
                        yield pltpu.make_async_copy(
                            o_refs[2 * s + side].at[order_ref[g * group + j]],
                            o_ref.at[g, pl.ds(j * qc, qc), pl.ds(at, half)], sems.at[g])

        @pl.when(step == 0)
        def _():
            for g in range(seqs // group):
                for c in copies(g):
                    c.start()

        for c in copies(step):
            c.wait()
        sq = jnp.zeros((rows, 1), F32)
        for f in range(shards):
            a = dot(o_ref[step], w_ref[f].reshape(width, cols)).astype(BF16)
            a_ref[:, f * cols:(f + 1) * cols] = a
            a = a.astype(F32)
            sq += jnp.sum(a * a, axis=-1, keepdims=True)
        inv = lax.rsqrt(sq / width + NORM_EPS)
        for j, x_ref in enumerate((x0_ref, x1_ref)):
            r = slice(j * qc, (j + 1) * qc)
            for f in range(shards):
                c = slice(f * cols, (f + 1) * cols)
                h_ref = (ha_ref, hb_ref)[f // (shards // 2)]
                hc = slice(f % (shards // 2) * cols, (f % (shards // 2) + 1) * cols)
                h_ref[j, :, hc] = (x_ref[0, :, c].astype(F32) + a_ref[r, c].astype(F32) * inv[r] * gain_ref[:, c]).astype(BF16)

    x_spec = lambda j: pl.BlockSpec((1, qc, width), lambda g, order: (order[g * group + j], chunk, 0))
    return pl.pallas_call(
        body,
        grid_spec=pltpu.PrefetchScalarGridSpec(
            num_scalar_prefetch=1, grid=(seqs // group,),
            in_specs=[pl.BlockSpec(memory_space=pl.ANY)] * (2 * sources) + [
                pl.BlockSpec(w.shape, lambda g, order: (0, 0, 0, 0), pipeline_mode=pl.Buffered(1)), x_spec(0), x_spec(1),
                pl.BlockSpec((1, width), lambda g, order: (0, 0))],
            out_specs=[pl.BlockSpec((group, qc, width // 2), lambda g, order: (g, 0, 0))] * 2,
            scratch_shapes=[pltpu.VMEM((seqs // group, rows, width), BF16), pltpu.VMEM((rows, width), BF16),
                            pltpu.SemaphoreType.DMA((seqs // group,))]),
        out_shape=[jax.ShapeDtypeStruct((seqs, qc, width // 2), BF16)] * 2,
        compiler_params=params(), cost_estimate=cost(2 * seqs * qc * width * width, 6 * seqs * qc * width + 2 * width * width))(order, *outs, w, x, x, gain)


def mlp_up(hs, w, gate_spec, up_spec, first, steps):
    seqs = len(hs)
    qc, half = hs[0][0].shape[-2:]
    width = 2 * half
    tn = 256
    group = 2
    rows = seqs * qc

    def body(*refs):
        h_refs, (g_ref, u_ref, act_ref, h_ref, sems) = refs[:2 * seqs], refs[2 * seqs:]
        step = pl.program_id(0)

        def copies(p):
            for q in range(group):
                n = p * group + q
                for side in range(2):
                    src = h_refs[2 * n + side]
                    src = src if hs[n][2] is None else src.at[hs[n][2]]
                    yield pltpu.make_async_copy(src, h_ref.at[pl.ds(n * qc, qc), pl.ds(side * half, half)], sems.at[p])

        @pl.when(step == 0)
        def _():
            for p in range(seqs // group):
                for c in copies(p):
                    c.start()

        g = g_ref[...].reshape(width, tn)
        u = u_ref[...].reshape(width, tn)
        for p in range(seqs // group):
            @pl.when(step == 0)
            def _(p=p):
                for c in copies(p):
                    c.wait()

            r = slice(p * group * qc, (p + 1) * group * qc)
            gate = dot(h_ref[r, :], g)
            up = dot(h_ref[r, :], u)
            act_ref[r, :] = (jax.nn.silu(gate) * up).astype(BF16)

    index = lambda i: first + i
    flat = [a for pair in hs for a in pair[:2]]
    return pl.pallas_call(
        body, grid=(steps,),
        in_specs=[pl.BlockSpec(memory_space=pl.ANY)] * (2 * seqs) + [gate_spec(index), up_spec(index)],
        out_specs=pl.BlockSpec((rows, tn), lambda i: (0, i)),
        out_shape=jax.ShapeDtypeStruct((rows, steps * tn), BF16),
        scratch_shapes=[pltpu.VMEM((rows, width), BF16), pltpu.SemaphoreType.DMA((seqs // group,))],
        compiler_params=params(), cost_estimate=cost(4 * rows * width * steps * tn, 2 * rows * width + 4 * width * steps * tn))(*flat, w, w)


def mlp_down(acts, w, down_spec, seqs, width):
    rows = acts[0].shape[0]
    qc = rows // seqs
    ff = sum(a.shape[1] for a in acts)
    n = len(acts)
    tn = 256
    half = width // 2
    per_side = half // tn
    group = 2

    def body(*refs):
        act_refs, d_ref, outs, act_ref, sems = refs[:n], refs[n], refs[n + 1:-2], refs[-2], refs[-1]
        step = pl.program_id(0)

        def copies(p):
            at = 0
            r = pl.ds(p * group * qc, group * qc)
            for a, ref in zip(acts, act_refs):
                yield pltpu.make_async_copy(ref.at[r, :], act_ref.at[r, pl.ds(at, a.shape[1])], sems.at[p])
                at += a.shape[1]

        @pl.when(step == 0)
        def _():
            for p in range(seqs // group):
                for c in copies(p):
                    c.start()

        d = d_ref[...].reshape(ff, tn)
        for p in range(seqs // group):
            @pl.when(step == 0)
            def _(p=p):
                for c in copies(p):
                    c.wait()

            m = dot(act_ref[p * group * qc:(p + 1) * group * qc, :], d).astype(BF16)
            for side in range(2):
                @pl.when(step // per_side == side)
                def _(side=side, m=m, p=p):
                    for q in range(group):
                        outs[2 * (p * group + q) + side][...] = m[q * qc:(q + 1) * qc]

    first = pl.BlockSpec((qc, tn), lambda i: (0, jnp.minimum(i, per_side - 1)))
    second = pl.BlockSpec((qc, tn), lambda i: (0, jnp.maximum(i - per_side, 0)))
    return pl.pallas_call(
        body, grid=(2 * per_side,),
        in_specs=[pl.BlockSpec(memory_space=pl.ANY)] * n + [down_spec(lambda i: i)],
        out_specs=[first, second] * seqs,
        out_shape=[jax.ShapeDtypeStruct((qc, half), BF16)] * (2 * seqs),
        scratch_shapes=[pltpu.VMEM((rows, ff), BF16), pltpu.SemaphoreType.DMA((seqs // group,))],
        compiler_params=params(), cost_estimate=cost(2 * rows * width * ff, 2 * rows * (width + ff) + 2 * width * ff))(*acts, w)


def finish(parts_a, parts_b, h_a, h_b, gain, place, whole):
    rows, half = h_a.shape[-2:]
    width = 2 * half
    block = 256
    per_side = half // block
    tr = min(128, rows)
    n = len(parts_a)

    def body(*refs):
        pa, pb = refs[:n], refs[n:2 * n]
        h_refs, gain_ref, outs = refs[2 * n:2 * n + 2], refs[2 * n + 2], refs[2 * n + 3:]
        sums = []
        for side in (pa, pb):
            m = side[0][...].astype(F32)
            for p in side[1:]:
                m = m + p[...].astype(F32)
            sums.append(m.astype(BF16).astype(F32))
        sq = sum(jnp.sum(m * m, axis=-1, keepdims=True) for m in sums)
        inv = lax.rsqrt(sq / width + NORM_EPS)
        for side in range(2):
            for b in range(per_side):
                c = slice(b * block, (b + 1) * block)
                at = place(side, b)
                gain_cols = gain_ref[:, at * block:(at + 1) * block]
                val = (h_refs[side][0, :, c].astype(F32) + sums[side][:, c] * inv * gain_cols).astype(BF16)
                if whole:
                    outs[0][:, at * block:(at + 1) * block] = val
                else:
                    at_half = at % per_side
                    outs[at // per_side][:, at_half * block:(at_half + 1) * block] = val

    part = pl.BlockSpec((tr, half), lambda i: (i, 0))
    out_width = width if whole else half
    outs = 1 if whole else 2
    return pl.pallas_call(
        body, grid=(rows // tr,),
        in_specs=[part] * (2 * n) + [pl.BlockSpec((1, tr, half), lambda i: (0, i, 0))] * 2
        + [pl.BlockSpec((1, width), lambda i: (0, 0))],
        out_specs=[pl.BlockSpec((tr, out_width), lambda i: (i, 0))] * outs,
        out_shape=[jax.ShapeDtypeStruct((rows, out_width), BF16)] * outs,
        compiler_params=params(), cost_estimate=cost(rows * width * 2000, rows * width * 2 * (n + 2)))(*parts_a, *parts_b, *(h if h.ndim == 3 else h[None] for h in (h_a, h_b)), gain)


def qkv_full(x, w, q_gain, k_gain, cos_t, sin_t, part, chunk):
    tokens, width = x.shape
    shards, tps, _, cols = w.shape
    depth = width // shards
    per = part // cols

    def body(x_ref, w_ref, qg_ref, kg_ref, cos_ref, sin_ref, q_ref, k_ref, v_ref, q_raw, k_raw, q_sq, k_sq):
        which, t = pl.program_id(0), pl.program_id(1)

        def product(b):
            return dot(x_ref[...], w_ref[:, 0, b * depth:(b + 1) * depth, :].reshape(width, cols))

        def keep(raw, sq):
            total = jnp.where(t == 0, 0.0, sq[...])
            for b in range(per):
                out = product(b)
                raw[t, :, b * cols:(b + 1) * cols] = out
                total += jnp.sum(out * out, axis=-1, keepdims=True)
            sq[...] = total

        def rotated(raw, sq, gain_ref, dst):
            inv = lax.rsqrt(sq[...] / width + NORM_EPS)
            for h in range(part // HEAD_DIM):
                c = slice(h * HEAD_DIM, (h + 1) * HEAD_DIM)
                vals = raw[t, :, c] * inv * gain_ref[:, c]
                dst[0, :, c] = rotate(vals, cos_ref[...], sin_ref[...]).astype(BF16)

        @pl.when(which == 0)
        def _():
            keep(q_raw, q_sq)

        @pl.when(which == 1)
        def _():
            keep(k_raw, k_sq)
            rotated(q_raw, q_sq, qg_ref, q_ref)

        @pl.when(which == 2)
        def _():
            for b in range(per):
                v_ref[0, :, b * cols:(b + 1) * cols] = product(b).astype(BF16)
            rotated(k_raw, k_sq, kg_ref, k_ref)

    table = pl.BlockSpec((tokens, HEAD_DIM), lambda i, t: (chunk, 0), pipeline_mode=pl.Buffered(1))
    gain = pl.BlockSpec((1, part), lambda i, t: (0, t))
    late = pl.BlockSpec((1, tokens, part), lambda i, t: (jnp.where(i == 2, t, 0), 0, 0))
    return pl.pallas_call(
        body, grid=(3, tps),
        in_specs=[pl.BlockSpec((tokens, width), lambda i, t: (0, 0), pipeline_mode=pl.Buffered(1)),
                  pl.BlockSpec((shards, 1, per * depth, cols), lambda i, t: (0, t, i, 0)), gain, gain, table, table],
        out_specs=[pl.BlockSpec((1, tokens, part), lambda i, t: (jnp.where(i == 1, t, jnp.where(i == 0, 0, tps - 1)), 0, 0)), late, late],
        out_shape=[jax.ShapeDtypeStruct((tps, tokens, part), BF16)] * 3,
        scratch_shapes=[pltpu.VMEM((tps, tokens, part), F32)] * 2 + [pltpu.VMEM((tokens, 1), F32)] * 2,
        compiler_params=params("arbitrary", "arbitrary"),
        cost_estimate=cost(6 * tokens * width * width, 8 * tokens * width + 6 * width * width))(x, w, q_gain, k_gain, cos_t, sin_t)


def out_proj_full(o_a, o_b, w, row_block, depth, x, gain):
    tokens, width = x.shape
    shards, tps, _, cols = w.shape
    half = depth // 2
    group = 2
    tr = min(256, tokens)

    def body(oa_ref, ob_ref, w_ref, x_ref, gain_ref, ha_ref, hb_ref, o_ref, raw_ref, sq_ref):
        f = pl.program_id(0)

        @pl.when(f == 0)
        def _():
            for t in range(tps):
                o_ref[:, t * depth:t * depth + half] = oa_ref[t]
                o_ref[:, t * depth + half:(t + 1) * depth] = ob_ref[t]

        total = jnp.where(f == 0, 0.0, sq_ref[...])
        for b in range(group):
            out = dot(o_ref[...], w_ref[b].reshape(tps * depth, cols)).astype(BF16)
            raw_ref[f * group + b] = out
            out = out.astype(F32)
            total += jnp.sum(out * out, axis=-1, keepdims=True)
        sq_ref[...] = total

        @pl.when(f == shards // group - 1)
        def _():
            def rows_body(r, _):
                rows = pl.ds(r * tr, tr)
                inv = lax.rsqrt(sq_ref[rows, :] / width + NORM_EPS)
                for m in range(shards):
                    c = slice(m * cols, (m + 1) * cols)
                    dst = slice(m // 2 * cols, (m // 2 + 1) * cols)
                    (ha_ref, hb_ref)[m % 2][rows, dst] = (
                        x_ref[rows, c].astype(F32) + raw_ref[m, rows, :].astype(F32) * inv * gain_ref[:, c]).astype(BF16)
                return 0

            lax.fori_loop(0, tokens // tr, rows_body, 0)

    fixed = lambda s: pl.BlockSpec(s, lambda f: (0,) * len(s), pipeline_mode=pl.Buffered(1))
    return pl.pallas_call(
        body, grid=(shards // group,),
        in_specs=[fixed(o_a.shape), fixed(o_b.shape), pl.BlockSpec((group, tps, depth, cols), lambda f: (f, 0, row_block, 0)),
                  fixed((tokens, width)), fixed((1, width))],
        out_specs=[pl.BlockSpec((tokens, width // 2), lambda f: (0, 0))] * 2,
        out_shape=[jax.ShapeDtypeStruct((tokens, width // 2), BF16)] * 2,
        scratch_shapes=[pltpu.VMEM((tokens, width), BF16), pltpu.VMEM((shards, tokens, cols), BF16), pltpu.VMEM((tokens, 1), F32)],
        compiler_params=params(),
        cost_estimate=cost(2 * tokens * width * width, 2 * width * (width + 2 * tokens)))(o_a, o_b, w, x, gain)


class Ring:
    def __init__(self, axis, size):
        assert size == 4
        self.axis, self.size = axis, size

    def up(self, a):
        return lax.ppermute(a, self.axis, [(i, (i + 1) % self.size) for i in range(self.size)])

    def down(self, a):
        return lax.ppermute(a, self.axis, [(i, (i - 1) % self.size) for i in range(self.size)])

    def far(self, a):
        return lax.ppermute(a, self.axis, [(i, (i + 2) % self.size) for i in range(self.size)])

    def collect(self, a):
        me = lax.axis_index(self.axis)
        out = jnp.zeros((self.size, *a.shape), a.dtype)
        pieces = [(0, a), (1, self.down(a)), (3, self.up(a)), (2, self.far(a))]
        for rel, piece in pieces:
            out = lax.dynamic_update_index_in_dim(out, piece, lax.rem(me + rel, self.size), 0)
        return out

    def exchange(self, pieces):
        me = lax.axis_index(self.axis)
        piece = lambda rel: lax.dynamic_index_in_dim(pieces, lax.rem(me + rel, self.size), 0, keepdims=False)
        got = [(0, piece(0)), (3, self.up(piece(1))), (1, self.down(piece(3))),
               (2, self.far(piece(2)))]
        out = jnp.zeros(pieces.shape, pieces.dtype)
        for rel, a in got:
            out = lax.dynamic_update_index_in_dim(out, a, lax.rem(me + rel, self.size), 0)
        return out

    def gather(self, a, b):
        below_a, above_b = self.up(a), self.down(b)
        below_b, above_a = self.up(b), self.down(a)
        far_a, far_b = self.up(below_a), self.down(above_b)
        return [(a, b), (above_a, above_b), (far_a, far_b), (below_a, below_b)]

    def scatter(self, parts):
        own_a, own_b, one_a, one_b, two_a, two_b, three_a, three_b = parts
        far_a, far_b = self.up(two_a), self.down(two_b)
        below_b, above_a = self.up(one_b), self.down(three_a)
        below_a = self.up(one_a + far_a)
        above_b = self.down(three_b + far_b)
        return [own_a, below_a, above_a], [own_b, below_b, above_b]


def solution(mesh):
    cores = 2
    dp, tp, fsdp = mesh.shape['dp'], mesh.shape['tp'], mesh.shape['fsdp']
    xs = fsdp // cores
    mesh = jax.sharding.Mesh(mesh.devices.reshape(dp, tp, xs, cores), ('dp', 'tp', 'x', 'c'))
    shards = ('x', 'c')
    batch_axes = ('dp', 'x', 'c')
    act_spec = P(batch_axes, None, None)
    in_cols = P(None, shards, 'tp')
    in_rows = P(None, 'tp', shards)
    tp_gain = P(None, 'tp')
    fsdp_gain = P(None, shards)
    cache_spec = P(None, batch_axes, None, 'tp', None)
    ring_y, ring_x = Ring('tp', tp), Ring('x', xs)

    def gather_all(a):
        g = lax.all_gather(a, ('x', 'c', 'tp'), axis=0, tiled=False)
        return g.reshape(fsdp, tp, *a.shape)

    def blocks_of(w, cols):
        return [w[:, i:i + cols] for i in range(0, w.shape[1], cols)]

    def local_layers(x, w_query, w_key, w_value, w_out, w_gate, w_up, w_down, q_norm_w, k_norm_w, attn_norm_w, ffn_norm_w):
        batch, seq_len, width = x.shape
        assert batch == tp and w_query.shape[0] == 2
        tokens = batch * seq_len
        qc = seq_len // CHUNKS
        part = w_query.shape[2]
        cols = w_out.shape[2]
        ff = w_gate.shape[2]
        per_side = width // 2 // cols
        cos_t, sin_t = rope_tables(seq_len)
        me = lax.axis_index('tp')
        seq_order = lax.rem(me + jnp.arange(tp, dtype=jnp.int32), tp)

        w_qkv = lax.all_gather(jnp.concatenate([w_query[0], w_key[0], w_value[0]], axis=1), shards, axis=0, tiled=True)
        fsdp_gains = lax.all_gather(jnp.stack([attn_norm_w, ffn_norm_w]), shards, axis=2, tiled=True)
        tp_gains = ring_y.collect(jnp.stack([q_norm_w[1], k_norm_w[1]]))
        q_gain1, k_gain1 = tp_gains[:, 0].reshape(1, width), tp_gains[:, 1].reshape(1, width)
        x, fsdp_gains, q_gain1, k_gain1 = lax.optimization_barrier((x, fsdp_gains, q_gain1, k_gain1))
        w_o0 = gather_all(w_out[0])
        w_gu0 = lax.all_gather(jnp.concatenate([w_gate[0], w_up[0]], axis=1), shards, axis=0, tiled=True)
        w_d0 = lax.all_gather(w_down[0], shards, axis=0, tiled=False)
        w_attn1 = jnp.concatenate(
            blocks_of(w_query[1], cols) + blocks_of(w_key[1], cols) + blocks_of(w_value[1], cols) + [w_out[1]], axis=0)
        w_attn1 = lax.all_gather(ring_y.collect(w_attn1), shards, axis=0, tiled=False)
        share = ff // xs
        pieces = [jnp.concatenate(blocks_of(w_gate[1][:, i * share:(i + 1) * share], cols)
                                  + blocks_of(w_up[1][:, i * share:(i + 1) * share], cols)
                                  + [w_down[1][i * share:(i + 1) * share]], axis=0) for i in range(xs)]
        mlp1 = ring_x.exchange(jnp.stack(pieces))
        mlp1 = lax.all_gather(mlp1, ('c', 'tp'), axis=0, tiled=False)
        mlp1 = mlp1.reshape(cores, tp, *mlp1.shape[1:])
        depth = w_gate.shape[1]
        up_rows = share // cols * depth

        q_raw, k_raw, values, sq = qkv_raw(x.reshape(tokens, width), w_qkv)
        sq_up, sq_down = ring_y.up(sq), ring_y.down(sq)
        sq_far = lax.ppermute(sq, 'tp', [(i, (i + 2) % tp) for i in range(tp)])
        inv = lax.rsqrt((sq + sq_up + sq_down + sq_far) / width + NORM_EPS)
        queries, keys_rot = norm_rope(q_raw, k_raw, inv, q_norm_w[:1], k_norm_w[:1], cos_t, sin_t)
        shape3 = (batch, seq_len, part)
        queries, keys_rot, values = (a.reshape(shape3) for a in (queries, keys_rot, values))

        def mlp(hs, w, gate, up, w_down, down, ff):
            steps = ff // 256 // 2
            acts = [mlp_up(hs, w, gate, up, i * steps, steps) for i in range(2)]
            return mlp_down(acts, w_down, down, len(hs), width)

        def cols_spec(offset):
            return lambda index: pl.BlockSpec((width, 256), lambda i: (0, offset + index(i)))

        gate0, up0 = cols_spec(0), cols_spec(ff // 256)
        down0 = lambda index: pl.BlockSpec((1, ff, cols), lambda i: (index(i), 0, 0))
        gathered = []
        for c in range(CHUNKS):
            own = attention(queries, c, qc, [(keys_rot, values, qc * (c + 1))])
            gathered.append(ring_y.gather(*own))
        sums, own_h = [], []
        for c in range(CHUNKS):
            outs = [a for pair in gathered[c] for a in pair]
            h_a, h_b = out_proj_gathered(seq_order, outs, w_o0, x, fsdp_gains[0, :1], c)
            sums.append(mlp([(h_a, h_b, s) for s in range(batch)], w_gu0, gate0, up0, w_d0, down0, ff))
            own_h.append((h_a, h_b))

        def up_spec(block):
            return lambda index: pl.BlockSpec((cores, 1, xs, depth, 256),
                                              lambda i: (0, index(i) // (share // 256), 0, block + index(i) % (share // 256), 0))

        gate1, up1 = up_spec(0), up_spec(share // 256)
        down1 = lambda index: pl.BlockSpec((1, tp, 1, share, cols), lambda i: (index(i) // xs, 0, index(i) % xs, 2 * up_rows // share, 0))
        kvs, caches, h1, gathered = [], [], [], []
        for c in range(CHUNKS):
            sum_a, sum_b = ring_y.scatter(sums[c])
            hidden, = finish(sum_a, sum_b, *own_h[c], fsdp_gains[1, :1], lambda side, b: side * per_side + b, True)
            q1, k1, v1 = qkv_full(hidden, w_attn1, q_gain1, k_gain1, cos_t, sin_t, part, c)
            caches.append([lax.all_to_all(a, 'tp', split_axis=0, concat_axis=0, tiled=True) for a in (k1, v1)])
            kvs.append((k1, v1, qc))
            own = attention(q1, 0, qc, list(kvs))
            h1.append(out_proj_full(*own, w_attn1, 3 * part * depth // cols // w_out.shape[1], w_out.shape[1], hidden,
                                    fsdp_gains[0, 1:]))
            gathered.append(ring_x.gather(*h1[-1]))
        sums = []
        for c in range(CHUNKS):
            hs = gathered[c]
            if c == CHUNKS - 1:
                hs, caches = lax.optimization_barrier((hs, caches))
            sums.append(mlp([(*pair, None) for pair in hs], mlp1, gate1, up1, mlp1, down1, tp * share))
        layers5 = lambda a: a.reshape(1, batch, seq_len, part // HEAD_DIM, HEAD_DIM)
        caches = [jnp.concatenate([caches[c][n] for c in range(CHUNKS)], axis=1) for n in range(2)]
        first = lax.optimization_barrier((keys_rot, values, sums[-1][0]))[:2]
        first = lax.optimization_barrier([layers5(a) for a in first])
        y = jnp.zeros(x.shape, BF16)
        for c in range(CHUNKS):
            sum_a, sum_b = ring_x.scatter(sums[c])
            y_own = finish(sum_a, sum_b, *h1[c], fsdp_gains[1, 1:], lambda side, b: 2 * b + side, False)
            for rel, pair in enumerate(ring_y.gather(*y_own)):
                for side in range(2):
                    y = lax.dynamic_update_slice(y, pair[side][None], (seq_order[rel], c * qc, side * width // 2))

            if c < CHUNKS - 1:
                second = lax.optimization_barrier((*caches, y_own[0]))[:2]
                second = lax.optimization_barrier([layers5(a) for a in second])
            else:
                first = lax.optimization_barrier((*first, y_own[0]))[:2]
        return y, *(jnp.concatenate([a, b], axis=0) for a, b in zip(first, second))

    return jax.shard_map(local_layers, mesh=mesh,
                         in_specs=(act_spec, in_cols, in_cols, in_cols, in_rows, in_cols, in_cols, in_rows,
                                   tp_gain, tp_gain, fsdp_gain, fsdp_gain),
                         out_specs=(act_spec, cache_spec, cache_spec), check_vma=False)
```
